32 devices in a mesh: member: 2 (over y), lon: 8 (over z, x), lat: 2 (over core).
Axes of the slice: x: 2, y: 2, z: 4, core: 2. Of those that a mesh axis runs over, the one named last changes fastest.
Arguments:
- state_tokens: bfloat16 [8, 24, 96, 768], P('member', 'lat', 'lon'), parts along dimension 0, may hold values from -32 to 32
- land_mask: int32 [24, 96], P('lat', 'lon'), may hold values 0 or 1
- pad_mask: int32 [24], replicated, may hold values from 0 to 1, as said below
- land_embed: float32 [2, 768], replicated, may hold values from -3 to 3
- w_qkv: bfloat16 [768, 1152], replicated, may hold values from -0.21875 to 0.21875
- w_proj: bfloat16 [384, 768], replicated, may hold values from -0.3125 to 0.3125
- proj_bias: float32 [768], replicated, may hold values from -4 to 4
- norm_gain: float32 [768], replicated, may hold values from 0.5 to 1.5
- norm_shift: float32 [768], replicated, may hold values from -1.5 to 1.5
- bias_table: bfloat16 [4, 2, 12, 3312], P('lat'), may hold values from -3.5 to 320
- index_table: int32 [144, 144], replicated, may hold values from 0 to 3311
Outputs:
- result: bfloat16 [8, 24, 96, 768], P('member', 'lat', 'lon'), parts along dimension 0
The draws below stay inside these ranges and needn't reach their ends.
There are 2 independent parts, one for each index of `member`. The reference program is written for one: setup_inputs(seed, part) draws one part's arguments, and reference() takes and returns one part's arrays. A program takes and returns all parts, laid end to end along the dimension named above; an argument that names none is the same for every part. Nothing has to cross between parts.
Inputs may be any that keep to these rules, and one draw needn't show every extreme that they name: pad_mask is 1 on every row except at most the first 2 and the last 2 of the 24 rows, which are 0 where padded; one of the two ends has exactly 2 padding rows.
All inputs are finite; a program needn't handle non-finite values. No bound on the sum of `land_mask` on one device may be relied on, other than what follows from the above.
Results may differ from the reference program's by a relative error of at most 0.0085.
Values may be sent and summed in bfloat16 or wider, within the bound.
No kernel may reach another device: no remote copies, remote signals or barrier semaphores. Data moves between devices by JAX's collectives and lax.ppermute only.
A program may use at most 64 MiB of HBM per device.

```python
import jax
import jax.numpy as jnp
from jax import lax

D = 768
HEADS = 12
HEAD_DIM = 32
WIN_Z = 2
WIN_LAT = 6
WIN_LON = 12
LEVELS = 4
WIN_TOK = 144
BIAS_POS = 3312
LAT = 24
LON = 96
LAT_WIN = 4
Z_WIN = 2


def index_helper(key):
    return jax.random.randint(jax.random.fold_in(key, 11), (WIN_TOK, WIN_TOK), 0, BIAS_POS, dtype=jnp.int32)


def draw_index_table(key, part):
    return index_helper(key)


def draw_bias_table(key, part):
    inner_key = jax.random.fold_in(key, 23)
    full_shape = (LAT_WIN, Z_WIN, HEADS, BIAS_POS)
    entries = jnp.clip(jax.random.normal(inner_key, full_shape, jnp.float32), -3.5, 3.5)
    return entries.astype(jnp.bfloat16)


def draw_state_tokens(key, part):
    subkeys = jax.random.split(jax.random.fold_in(key, 5), 3)
    full_shape = (LEVELS, LAT, LON, D)
    normal_part = jnp.clip(jax.random.normal(subkeys[0], full_shape, jnp.float32), -3.5, 3.5)
    row_scale = jnp.exp(jax.random.uniform(subkeys[1], (LEVELS, LAT, LON, 1), jnp.float32, jnp.log(0.3), jnp.log(3.0)))
    column_scale = jnp.exp(jax.random.uniform(subkeys[2], (D,), jnp.float32, jnp.log(0.3), jnp.log(3.0)))
    drawn_values = normal_part * row_scale * column_scale
    return drawn_values.astype(jnp.bfloat16)


def draw_pad_mask(key, part):
    subkeys = jax.random.split(jax.random.fold_in(key, 31), 2)
    other_end = jax.random.randint(subkeys[0], (), 0, 3, dtype=jnp.int32)
    chosen = jax.random.randint(subkeys[1], (), 0, 2, dtype=jnp.int32)
    north_rows = jnp.where(chosen == 0, 2, other_end)
    south_rows = jnp.where(chosen == 0, other_end, 2)
    positions = jnp.arange(LAT, dtype=jnp.int32)
    row_mask = (positions >= north_rows) & (positions < LAT - south_rows)
    return row_mask.astype(jnp.int32)


def place_ends(result, rng, smallest, high):
    spot = [jax.random.randint(jax.random.fold_in(rng, axis), (), 0, length) for axis, length in enumerate(result.shape)]
    main_axis = result.shape.index(max(result.shape))
    neighbour = spot[:main_axis] + [(spot[main_axis] + 1) % result.shape[main_axis]] + spot[main_axis + 1:]
    return result.at[tuple(spot)].set(smallest).at[tuple(neighbour)].set(high)


def scatter_about(own_key, extent, width, bound, held_as=jnp.bfloat16):
    return jnp.clip(width * jax.random.normal(own_key, extent, jnp.float32), -bound, bound).astype(held_as)


def setup_inputs(seed: int = 0, part: int = 0) -> dict:
    seeds = jax.random.split(jax.random.key(seed), 12)
    part_splits = jax.random.split(jax.random.fold_in(seeds[11], part), 12)
    state_tokens = draw_state_tokens(jax.random.fold_in(jax.random.fold_in(seeds[11], part), 71), part)
    land_mask = place_ends((jax.random.randint(seeds[1], (LAT, LON), 0, 3) < 1).astype(jnp.int32), jax.random.fold_in(seeds[1], 1), 0, 1)
    pad_mask = draw_pad_mask(jax.random.fold_in(seeds[11], 71), part)
    land_embed = scatter_about(seeds[3], (2, D), 0.5, 3.0, jnp.float32)
    w_qkv = scatter_about(seeds[4], (D, 3 * HEADS * HEAD_DIM), D ** -0.5, 0.21875)
    w_proj = scatter_about(seeds[5], (HEADS * HEAD_DIM, D), (HEADS * HEAD_DIM) ** -0.5, 0.3125)
    proj_bias = scatter_about(seeds[6], (D,), 1.0, 4.0, jnp.float32)
    norm_gain = jnp.clip(1.0 + 0.1 * jax.random.normal(seeds[7], (D,), jnp.float32), 0.5, 1.5)
    norm_shift = scatter_about(seeds[8], (D,), 0.3, 1.5, jnp.float32)
    bias_table = draw_bias_table(jax.random.fold_in(seeds[11], 71), part)
    index_table = draw_index_table(jax.random.fold_in(seeds[11], 71), part)
    return dict(state_tokens=state_tokens, land_mask=land_mask, pad_mask=pad_mask, land_embed=land_embed, w_qkv=w_qkv, w_proj=w_proj, proj_bias=proj_bias, norm_gain=norm_gain, norm_shift=norm_shift, bias_table=bias_table, index_table=index_table)


norm_epsilon = 1e-05

def region_of(position, length, window):
    half_window = window // 2
    return jnp.where(position < length - window, 0, jnp.where(position < length - half_window, 1, 2)).astype(jnp.int32)

def window_rules(levels, lat_start, lat_rows, lat_total, pad_mask):
    tokens = jnp.arange(WIN_TOK, dtype=jnp.int32)
    level_offset = tokens // (WIN_LAT * WIN_LON)
    row_offset = tokens // WIN_LON % WIN_LAT
    level_index = jnp.arange(levels // WIN_Z, dtype=jnp.int32)[:, None] * WIN_Z + level_offset[None, :]
    row_index = lat_start + jnp.arange(lat_rows // WIN_LAT, dtype=jnp.int32)[:, None] * WIN_LAT + row_offset[None, :]
    region = region_of(level_index, levels, WIN_Z)[:, None, :] * 3 + region_of(row_index, lat_total, WIN_LAT)[None, :, :]
    source_row = (row_index + WIN_LAT // 2) % lat_total
    lookup = (source_row[:, :, None] == jnp.arange(lat_total, dtype=jnp.int32)[None, None, :]).astype(jnp.int32)
    usable = lax.optimization_barrier(jnp.sum(lookup * pad_mask[None, None, :], axis=-1)) == 1
    return (region[:, :, :, None] == region[:, :, None, :]) & usable[None, :, None, :]

def earth_bias(bias_table, index_table):
    gathered = jnp.take(bias_table, index_table, axis=3).astype(jnp.float32)
    return jnp.transpose(gathered, (1, 0, 2, 3, 4))

def to_windows(layout):
    levels, lat_rows, lon_columns, channels = layout.shape
    shaped = layout.reshape(levels // WIN_Z, WIN_Z, lat_rows // WIN_LAT, WIN_LAT, lon_columns // WIN_LON, WIN_LON, channels)
    shaped = shaped.transpose(0, 2, 4, 1, 3, 5, 6)
    return shaped.reshape(levels // WIN_Z, lat_rows // WIN_LAT, lon_columns // WIN_LON, WIN_TOK, channels)

def from_windows(window_tiles):
    z_windows, lat_windows, lon_windows, tokens, channels = window_tiles.shape
    shaped = window_tiles.reshape(z_windows, lat_windows, lon_windows, WIN_Z, WIN_LAT, WIN_LON, channels)
    shaped = shaped.transpose(0, 3, 1, 4, 2, 5, 6)
    return shaped.reshape(z_windows * WIN_Z, lat_windows * WIN_LAT, lon_windows * WIN_LON, channels)

def attend(projections, bias_full, allowed):
    pieces = projections.astype(jnp.float32).reshape(projections.shape[:-1] + (3, HEADS, HEAD_DIM))
    queries = pieces[..., 0, :, :]
    key_rows = pieces[..., 1, :, :]
    value_rows = pieces[..., 2, :, :]
    scores = jnp.einsum('abthd,abuhd->abhtu', queries, key_rows) / jnp.sqrt(jnp.float32(HEAD_DIM)) + bias_full
    scores = jnp.where(allowed[:, :, None], scores, -jnp.inf)
    largest = lax.optimization_barrier(jnp.max(scores, axis=-1, keepdims=True))
    powers = jnp.exp(scores - largest)
    weights = (powers / lax.optimization_barrier(jnp.sum(powers, axis=-1, keepdims=True))).astype(jnp.bfloat16)
    attended = jnp.einsum('abhtu,abuhd->abthd', weights.astype(jnp.float32), value_rows).astype(jnp.bfloat16)
    return attended.reshape(attended.shape[:3] + (HEADS * HEAD_DIM,))

def finish(attended, w_proj, proj_bias, norm_gain, norm_shift):
    projected = jnp.dot(attended, w_proj, preferred_element_type=jnp.float32) + proj_bias
    average = lax.optimization_barrier(jnp.mean(projected, axis=-1, keepdims=True))
    centered = projected - average
    spread = lax.optimization_barrier(jnp.mean(centered * centered, axis=-1, keepdims=True))
    return centered * lax.rsqrt(spread + norm_epsilon) * norm_gain + norm_shift

def reference(state_tokens, land_mask, pad_mask, land_embed, w_qkv, w_proj, proj_bias, norm_gain, norm_shift, bias_table, index_table):
    embedded = jnp.where(land_mask[:, :, None] == 1, land_embed[1], land_embed[0])
    hidden = (state_tokens.astype(jnp.float32) + embedded[None]).astype(jnp.bfloat16)
    shifted = jnp.roll(hidden, (-(WIN_Z // 2), -(WIN_LAT // 2), -(WIN_LON // 2)), axis=(0, 1, 2))
    windows = jnp.moveaxis(to_windows(shifted), 2, 0)
    bias_full = earth_bias(bias_table, index_table)
    allowed = window_rules(LEVELS, 0, LAT, LAT, pad_mask)

    def one_column(column_block):
        projections = jnp.dot(column_block, w_qkv, preferred_element_type=jnp.float32).astype(jnp.bfloat16)
        return finish(attend(projections, bias_full, allowed), w_proj, proj_bias, norm_gain, norm_shift)
    normed = lax.map(one_column, windows)
    layout = from_windows(jnp.moveaxis(normed, 0, 2))
    restored = jnp.roll(layout, (WIN_Z // 2, WIN_LAT // 2, WIN_LON // 2), axis=(0, 1, 2))
    return (hidden.astype(jnp.float32) + restored).astype(jnp.bfloat16)
```

```python
import functools

import jax
import jax.numpy as jnp
from jax import lax
from jax.experimental import pallas as pl
from jax.experimental.pallas import tpu as pltpu
from jax.sharding import PartitionSpec as P

HEADS = 12
HEAD_DIM = 32
WIN_Z = 2
WIN_LAT = 6
WIN_LON = 12
WIN_TOK = 144
HALF_TOK = 72
LANES = 128
REST = WIN_TOK - LANES
LOW = 256

norm_epsilon = 1e-05


def from_behind(shard, axis, by):
    size = lax.axis_size(axis)
    return lax.ppermute(shard, axis, [(i, (i + by) % size) for i in range(size)])


def region_of(position, length, window):
    half_window = window // 2
    return jnp.where(
        position < length - window, 0, jnp.where(position < length - half_window, 1, 2)
    ).astype(jnp.int32)


def half_major(table, axis):
    shape = table.shape
    half = WIN_LON // 2
    split = shape[:axis] + (WIN_Z * WIN_LAT, 2, half) + shape[axis + 1:]
    return jnp.swapaxes(table.reshape(split), axis, axis + 1).reshape(shape)


def window_rules(levels, lat_start, lat_rows, lat_total, pad_mask):
    tokens = jnp.arange(HALF_TOK, dtype=jnp.int32)
    half = WIN_LON // 2
    level_offset = jnp.tile(tokens // (WIN_LAT * half), 2)
    row_offset = jnp.tile(tokens // half % WIN_LAT, 2)
    level_index = (
        jnp.arange(levels // WIN_Z, dtype=jnp.int32)[:, None] * WIN_Z + level_offset[None, :]
    )
    row_index = (
        lat_start
        + jnp.arange(lat_rows // WIN_LAT, dtype=jnp.int32)[:, None] * WIN_LAT
        + row_offset[None, :]
    )
    region = (
        region_of(level_index, levels, WIN_Z)[:, None, :] * 3
        + region_of(row_index, lat_total, WIN_LAT)[None, :, :]
    )
    source_row = (row_index + WIN_LAT // 2) % lat_total
    lookup = (
        source_row[:, :, None] == jnp.arange(lat_total, dtype=jnp.int32)[None, None, :]
    ).astype(jnp.int32)
    usable = jnp.sum(lookup * pad_mask[None, None, :], axis=-1) == 1
    key_code = jnp.where(usable[None], region, -1)
    return key_code[:, :, :, None], region[:, :, None, :]


def bias_kernel(table_ref, low_ref, high_ref, main_ref, rest_ref, *, tables, chunks, main_tiles, rest_tiles):
    position = lax.broadcasted_iota(jnp.int32, (LOW, LOW), 0)

    def pick(i):
        one_hot = jnp.where(position == low_ref[i], 1.0, 0.0).astype(jnp.bfloat16)
        found = jnp.dot(table_ref[...], one_hot, preferred_element_type=jnp.float32)
        high = high_ref[i]
        chosen = found[:tables]
        for c in range(1, chunks):
            chosen = jnp.where(high == c, found[c * tables:(c + 1) * tables], chosen)
        return chosen

    def main_step(i, carry):
        chosen = pick(i)
        main_ref[pl.ds(2 * i, tables, stride=WIN_TOK), :] = chosen[:, :LANES]
        main_ref[pl.ds(2 * i + 1, tables, stride=WIN_TOK), :] = chosen[:, LANES:]
        return carry

    def rest_step(i, carry):
        chosen = pick(main_tiles + i)
        per_half = LANES // REST
        for j in range(2 * per_half):
            part = chosen[:, :LANES] if j < per_half else chosen[:, LANES:]
            shift = (j % per_half) * REST
            if shift:
                part = pltpu.roll(part, LANES - shift, 1)
            rest_ref[pl.ds(2 * per_half * i + j, tables, stride=WIN_TOK), :] = part
        return carry

    lax.fori_loop(0, main_tiles, main_step, 0)
    lax.fori_loop(0, rest_tiles, rest_step, 0)


def earth_bias(bias_table, index_table):
    lat_windows, z_windows, heads, positions = bias_table.shape
    tables = lat_windows * z_windows * heads
    chunks = -(-positions // LOW)
    rows = bias_table.reshape(tables, positions)
    rows = jnp.pad(rows, ((0, 0), (0, chunks * LOW - positions)))
    rows = jnp.swapaxes(rows.reshape(tables, chunks, LOW), 0, 1).reshape(chunks * tables, LOW)
    index = half_major(half_major(index_table.T, 0), 1)
    main = index[:, :LANES].reshape(-1, 1, LOW)
    rest = index[:, LANES:].reshape(-1, 1, LOW)
    index = jnp.concatenate([main, rest], axis=0)
    out = jax.ShapeDtypeStruct((tables * WIN_TOK, LANES), jnp.float32)
    main_bias, rest_bias = pl.pallas_call(
        functools.partial(
            bias_kernel, tables=tables, chunks=chunks,
            main_tiles=main.shape[0], rest_tiles=rest.shape[0],
        ),
        out_shape=(out, out),
        compiler_params=pltpu.CompilerParams(vmem_limit_bytes=40 << 20),
        cost_estimate=pl.CostEstimate(
            flops=2 * chunks * tables * LOW * WIN_TOK * WIN_TOK,
            transcendentals=0, bytes_accessed=8 << 20,
        ),
        name="bias_lookup",
    )(rows, index % LOW, index // LOW)
    shape = (lat_windows, z_windows, heads, WIN_TOK, LANES)
    return main_bias.reshape(shape), rest_bias.reshape(shape)


def attend_kernel(
    own_ref, halo_ref, w_qkv_ref, main_ref, rest_ref, key_ref, query_ref, w_proj_ref,
    proj_bias_ref, gain_ref, shift_ref, out_own_ref, out_halo_ref, qkv_own, qkv_halo, attended_ref,
):
    windows = own_ref.shape[0]
    features = own_ref.shape[2]
    width = HEADS * HEAD_DIM
    qkv_own[...] = jnp.dot(
        own_ref[...].reshape(windows * HALF_TOK, features), w_qkv_ref[...],
        preferred_element_type=jnp.float32,
    )
    qkv_halo[...] = jnp.dot(
        halo_ref[...].reshape(windows * HALF_TOK, features), w_qkv_ref[...],
        preferred_element_type=jnp.float32,
    )
    scale = 1.0 / (HEAD_DIM ** 0.5)
    per_group = LANES // HEAD_DIM
    for w in range(windows):
        rows = slice(w * HALF_TOK, (w + 1) * HALF_TOK)
        qkv = jnp.concatenate([qkv_own[rows], qkv_halo[rows]], axis=0)
        queries = qkv[:, :width].T.astype(jnp.bfloat16)
        key_rows = qkv[:, width:2 * width].astype(jnp.bfloat16)
        value_rows = qkv[:, 2 * width:].T.astype(jnp.bfloat16)
        allowed = key_ref[w] == query_ref[w]
        pieces = []
        for h in range(HEADS):
            group, spot = h // per_group, h % per_group
            query = queries[h * HEAD_DIM:(h + 1) * HEAD_DIM]
            blocks = [jnp.zeros((HEAD_DIM, WIN_TOK), jnp.bfloat16)] * per_group
            blocks[spot] = query
            scores = jnp.dot(
                key_rows[:, group * LANES:(group + 1) * LANES], jnp.concatenate(blocks, axis=0),
                preferred_element_type=jnp.float32,
            )
            bias = jnp.concatenate([main_ref[w, h], rest_ref[w, h][:, :REST]], axis=1)
            scores = jnp.where(allowed, scores * scale + bias, -1e30)
            powers = jnp.exp(scores - jnp.max(scores, axis=0, keepdims=True))
            weights = powers * (1.0 / jnp.sum(powers, axis=0, keepdims=True))
            pieces.append(jnp.dot(
                value_rows[h * HEAD_DIM:(h + 1) * HEAD_DIM], weights.astype(jnp.bfloat16),
                preferred_element_type=jnp.float32,
            ))
        attended_ref[w * WIN_TOK:(w + 1) * WIN_TOK] = (
            jnp.concatenate(pieces, axis=0).T.astype(jnp.bfloat16)
        )
    projected = jnp.dot(
        attended_ref[...], w_proj_ref[...], preferred_element_type=jnp.float32
    ) + proj_bias_ref[...]
    average = jnp.mean(projected, axis=-1, keepdims=True)
    centered = projected - average
    spread = jnp.mean(centered * centered, axis=-1, keepdims=True)
    normed = centered * lax.rsqrt(spread + norm_epsilon) * gain_ref[...] + shift_ref[...]
    for w in range(windows):
        start = w * WIN_TOK
        out_own_ref[w] = normed[start:start + HALF_TOK].astype(jnp.bfloat16)
        out_halo_ref[w] = normed[start + HALF_TOK:start + WIN_TOK].astype(jnp.bfloat16)


def attend(own, halo, z, w_qkv, bias, codes, w_proj, proj_bias, norm_gain, norm_shift):
    windows, _, features = own.shape
    main_bias, rest_bias = bias

    def whole(a):
        return pl.BlockSpec(a.shape, lambda i: (0,) * a.ndim)

    bias_spec = pl.BlockSpec((windows, None, HEADS, WIN_TOK, LANES), lambda i: (0, z, 0, 0, 0))
    rows = [v.reshape(1, features) for v in (proj_bias, norm_gain, norm_shift)]
    args = (own, halo, w_qkv, main_bias, rest_bias, codes[0][z], codes[1][z], w_proj, *rows)
    specs = [whole(a) for a in args]
    specs[3] = specs[4] = bias_spec
    out = jax.ShapeDtypeStruct(own.shape, jnp.bfloat16)
    width = HEADS * HEAD_DIM
    return pl.pallas_call(
        attend_kernel,
        out_shape=(out, out),
        grid=(1,),
        in_specs=specs,
        out_specs=[whole(out), whole(out)],
        scratch_shapes=[
            pltpu.VMEM((windows * HALF_TOK, 3 * width), jnp.float32),
            pltpu.VMEM((windows * HALF_TOK, 3 * width), jnp.float32),
            pltpu.VMEM((windows * WIN_TOK, width), jnp.bfloat16),
        ],
        compiler_params=pltpu.CompilerParams(vmem_limit_bytes=48 << 20),
        cost_estimate=pl.CostEstimate(
            flops=6 * 10 ** 9, transcendentals=10 ** 6, bytes_accessed=8 << 20
        ),
        name="window_attention",
    )(*args)


def to_windows(layout):
    levels, lat_rows, columns, channels = layout.shape
    shaped = layout.reshape(
        levels // WIN_Z, WIN_Z, lat_rows // WIN_LAT, WIN_LAT, columns, channels
    )
    shaped = shaped.transpose(0, 2, 1, 3, 4, 5)
    return shaped.reshape(levels // WIN_Z, lat_rows // WIN_LAT, HALF_TOK, channels)


def from_windows(tiles):
    z_windows, lat_windows, _, channels = tiles.shape
    shaped = tiles.reshape(z_windows, lat_windows, WIN_Z, WIN_LAT, WIN_LON // 2, channels)
    shaped = shaped.transpose(0, 2, 1, 3, 4, 5)
    return shaped.reshape(z_windows * WIN_Z, lat_windows * WIN_LAT, WIN_LON // 2, channels)


def on_device(
    state_tokens,
    land_mask,
    pad_mask,
    land_embed,
    w_qkv,
    w_proj,
    proj_bias,
    norm_gain,
    norm_shift,
    bias_table,
    index_table,
):
    levels, lat_rows, lon_columns, features = state_tokens.shape
    lat_total = lat_rows * lax.axis_size("lat")
    lat_start = lax.axis_index("lat") * lat_rows
    level_half = WIN_Z // 2
    lat_half = WIN_LAT // 2
    lon_half = WIN_LON // 2

    def embed(tokens, mask):
        embedded = jnp.where(mask[:, :, None] == 1, land_embed[1], land_embed[0])
        return (tokens.astype(jnp.float32) + embedded[None]).astype(jnp.bfloat16)

    def shift_rows(part):
        rolled = jnp.roll(part, -level_half, axis=0)
        incoming = from_behind(rolled[:, :lat_half], "lat", -1)
        return to_windows(jnp.concatenate([rolled[:, lat_half:], incoming], axis=1))

    first = embed(state_tokens[:, :, :lon_half], land_mask[:, :lon_half])
    halo = from_behind(first, "lon", -1)
    last = embed(state_tokens[:, :, lon_half:], land_mask[:, lon_half:])
    own_windows = shift_rows(last)
    bias = earth_bias(bias_table, index_table)
    codes = window_rules(levels, lat_start, lat_rows, lat_total, pad_mask)
    halo_windows = shift_rows(halo)
    kept, returned = [], []
    for z in range(levels // WIN_Z):
        own_out, halo_out = attend(
            own_windows[z], halo_windows[z], z, w_qkv, bias, codes,
            w_proj, proj_bias, norm_gain, norm_shift,
        )
        kept.append(own_out)
        returned.append(from_behind(halo_out, "lon", 1))

    def unshift_rows(tiles):
        layout = from_windows(tiles)
        incoming = from_behind(layout[:, -lat_half:], "lat", 1)
        layout = jnp.concatenate([incoming, layout[:, :-lat_half]], axis=1)
        return jnp.roll(layout, level_half, axis=0).astype(jnp.float32)

    result_last = (last.astype(jnp.float32) + unshift_rows(jnp.stack(kept))).astype(jnp.bfloat16)
    result_first = (first.astype(jnp.float32) + unshift_rows(jnp.stack(returned))).astype(jnp.bfloat16)
    return jnp.concatenate([result_first, result_last], axis=2)


def solution(mesh):
    in_specs = (
        P("member", "lat", "lon", None),
        P("lat", "lon"),
        P(),
        P(),
        P(),
        P(),
        P(),
        P(),
        P(),
        P("lat", None, None, None),
        P(),
    )
    out_specs = P("member", "lat", "lon", None)
    return jax.shard_map(
        on_device, mesh=mesh, in_specs=in_specs, out_specs=out_specs, check_vma=False
    )
```

```python
import functools

import jax
import jax.numpy as jnp
import numpy as np
from jax import lax
from jax.experimental import pallas as pl
from jax.experimental.pallas import tpu as pltpu
from jax.sharding import PartitionSpec as P

HEADS = 12
HEAD_DIM = 32
WIN_Z = 2
WIN_LAT = 6
WIN_LON = 12
WIN_TOK = 144
HALF_TOK = 72
LANES = 128
REST = WIN_TOK - LANES
LOW = 256

norm_epsilon = 1e-05


def from_behind(shard, axis, by):
    size = lax.axis_size(axis)
    return lax.ppermute(shard, axis, [(i, (i + by) % size) for i in range(size)])


def region_of(position, length, window):
    half_window = window // 2
    return jnp.where(
        position < length - window, 0, jnp.where(position < length - half_window, 1, 2)
    ).astype(jnp.int32)


BLOCK = 36
SLAB = 16


def block_major(table):
    parts = (WIN_Z, 2, WIN_LAT // 2, 2, WIN_LON // 2)
    split = table.reshape(parts + parts)
    order = (3, 1, 0, 2, 4)
    return split.transpose(order + tuple(5 + o for o in order)).reshape(table.shape)


def offsets(groups):
    kept = -(-(groups - 1) * BLOCK // SLAB) * SLAB
    last = -(-BLOCK // SLAB) * SLAB
    starts = (0, kept, kept + last, 2 * kept + last)
    return starts, 2 * (kept + last)


def packing(lat_rows):
    third = WIN_LAT // 2
    groups = lat_rows // third
    starts, total = offsets(groups)
    chosen = np.zeros((total, WIN_Z * lat_rows * SLAB), np.float32)
    for half in range(2):
        for group in range(groups):
            first_row = 0 if group == groups - 1 else third * (group + 1)
            base = starts[2 * half + 1] if group == groups - 1 else starts[2 * half] + group * BLOCK
            for level in range(WIN_Z):
                for row in range(third):
                    for column in range(WIN_LON // 2):
                        packed = base + (level * third + row) * (WIN_LON // 2) + column
                        source = (level * lat_rows + first_row + row) * SLAB
                        chosen[packed, source + half * (WIN_LON // 2) + column] = 1
    return chosen


def window_rules(levels, lat_start, lat_rows, lat_total, pad_mask):
    tokens = jnp.arange(WIN_TOK, dtype=jnp.int32)
    third = WIN_LAT // 2
    level_offset = tokens // (BLOCK // WIN_Z) % WIN_Z
    row_offset = tokens // BLOCK % 2 * third + tokens // (WIN_LON // 2) % third
    level_index = (
        jnp.arange(levels // WIN_Z, dtype=jnp.int32)[:, None] * WIN_Z + level_offset[None, :]
    )
    row_index = (
        lat_start
        + jnp.arange(lat_rows // WIN_LAT, dtype=jnp.int32)[:, None] * WIN_LAT
        + row_offset[None, :]
    )
    region = (
        region_of(level_index, levels, WIN_Z)[:, None, :] * 3
        + region_of(row_index, lat_total, WIN_LAT)[None, :, :]
    )
    source_row = (row_index + WIN_LAT // 2) % lat_total
    lookup = (
        source_row[:, :, None] == jnp.arange(lat_total, dtype=jnp.int32)[None, None, :]
    ).astype(jnp.int32)
    usable = jnp.sum(lookup * pad_mask[None, None, :], axis=-1) == 1
    key_code = jnp.where(usable[None], region, -1)
    return key_code[:, :, :, None], region[:, :, None, :]


def bias_kernel(table_ref, low_ref, high_ref, main_ref, rest_ref, *, tables, chunks, main_tiles, rest_tiles):
    position = lax.broadcasted_iota(jnp.int32, (LOW, LOW), 0)

    def pick(i):
        one_hot = jnp.where(position == low_ref[i], 1.0, 0.0).astype(jnp.bfloat16)
        found = jnp.dot(table_ref[...], one_hot, preferred_element_type=jnp.float32)
        high = high_ref[i]
        chosen = found[:tables]
        for c in range(1, chunks):
            chosen = jnp.where(high == c, found[c * tables:(c + 1) * tables], chosen)
        return chosen

    def main_step(i, carry):
        chosen = pick(i)
        main_ref[pl.ds(2 * i, tables, stride=WIN_TOK), :] = chosen[:, :LANES]
        main_ref[pl.ds(2 * i + 1, tables, stride=WIN_TOK), :] = chosen[:, LANES:]
        return carry

    def rest_step(i, carry):
        chosen = pick(main_tiles + i)
        per_half = LANES // REST
        for j in range(2 * per_half):
            part = chosen[:, :LANES] if j < per_half else chosen[:, LANES:]
            shift = (j % per_half) * REST
            if shift:
                part = pltpu.roll(part, LANES - shift, 1)
            rest_ref[pl.ds(2 * per_half * i + j, tables, stride=WIN_TOK), :] = part
        return carry

    lax.fori_loop(0, main_tiles, main_step, 0, unroll=8)
    lax.fori_loop(0, rest_tiles, rest_step, 0, unroll=3)


def earth_bias(bias_table, index_table):
    lat_windows, z_windows, heads, positions = bias_table.shape
    tables = lat_windows * z_windows * heads
    chunks = -(-positions // LOW)
    rows = bias_table.reshape(tables, positions)
    rows = jnp.pad(rows, ((0, 0), (0, chunks * LOW - positions)))
    rows = jnp.swapaxes(rows.reshape(tables, chunks, LOW), 0, 1).reshape(chunks * tables, LOW)
    index = block_major(index_table.T)
    main = index[:, :LANES].reshape(-1, 1, LOW)
    rest = index[:, LANES:].reshape(-1, 1, LOW)
    index = jnp.concatenate([main, rest], axis=0)
    out = jax.ShapeDtypeStruct((tables * WIN_TOK, LANES), jnp.float32)
    main_bias, rest_bias = pl.pallas_call(
        functools.partial(
            bias_kernel, tables=tables, chunks=chunks,
            main_tiles=main.shape[0], rest_tiles=rest.shape[0],
        ),
        out_shape=(out, out),
        compiler_params=pltpu.CompilerParams(vmem_limit_bytes=40 << 20),
        cost_estimate=pl.CostEstimate(
            flops=2 * chunks * tables * LOW * WIN_TOK * WIN_TOK,
            transcendentals=0, bytes_accessed=8 << 20,
        ),
        name="bias_lookup",
    )(rows, index % LOW, index // LOW)
    shape = (lat_windows, z_windows, heads, WIN_TOK, LANES)
    return main_bias.reshape(shape), rest_bias.reshape(shape)


def attend_kernel(
    own_ref, own_last_ref, halo_ref, halo_last_ref, w_qkv_ref, main_ref, rest_ref, key_ref, query_ref, w_proj_ref,
    proj_bias_ref, gain_ref, shift_ref, out_own_ref, out_halo_ref, out_last_ref, qkv_ref, attended_ref,
):
    windows = main_ref.shape[0]
    width = HEADS * HEAD_DIM
    pieces = []
    for w in range(windows):
        for part, last in ((own_ref, own_last_ref), (halo_ref, halo_last_ref)):
            if w < windows - 1:
                pieces.append(part[w * HALF_TOK:(w + 1) * HALF_TOK])
            else:
                pieces.append(part[w * HALF_TOK:w * HALF_TOK + BLOCK])
                pieces.append(last[...])
    tokens = jnp.concatenate([p.astype(jnp.float32) for p in pieces], axis=0)
    qkv_ref[...] = jnp.dot(
        tokens.astype(jnp.bfloat16), w_qkv_ref[...], preferred_element_type=jnp.float32
    )
    scale = 1.0 / (HEAD_DIM ** 0.5)
    per_group = LANES // HEAD_DIM
    for w in range(windows):
        qkv = qkv_ref[w * WIN_TOK:(w + 1) * WIN_TOK]
        queries = qkv[:, :width].T.astype(jnp.bfloat16)
        key_rows = qkv[:, width:2 * width].astype(jnp.bfloat16)
        value_rows = qkv[:, 2 * width:].T.astype(jnp.bfloat16)
        allowed = key_ref[w] == query_ref[w]
        pieces = []
        for h in range(HEADS):
            group, spot = h // per_group, h % per_group
            query = queries[h * HEAD_DIM:(h + 1) * HEAD_DIM]
            blocks = [jnp.zeros((HEAD_DIM, WIN_TOK), jnp.bfloat16)] * per_group
            blocks[spot] = query
            scores = jnp.dot(
                key_rows[:, group * LANES:(group + 1) * LANES], jnp.concatenate(blocks, axis=0),
                preferred_element_type=jnp.float32,
            )
            bias = jnp.concatenate([main_ref[w, h], rest_ref[w, h][:, :REST]], axis=1)
            scores = jnp.where(allowed, scores * scale + bias, -1e30)
            powers = jnp.exp(scores - jnp.max(scores, axis=0, keepdims=True))
            weights = powers * (1.0 / jnp.sum(powers, axis=0, keepdims=True))
            pieces.append(jnp.dot(
                value_rows[h * HEAD_DIM:(h + 1) * HEAD_DIM], weights.astype(jnp.bfloat16),
                preferred_element_type=jnp.float32,
            ))
        attended_ref[w * WIN_TOK:(w + 1) * WIN_TOK] = (
            jnp.concatenate(pieces, axis=0).T.astype(jnp.bfloat16)
        )
    projected = jnp.dot(
        attended_ref[...], w_proj_ref[...], preferred_element_type=jnp.float32
    ) + proj_bias_ref[...]
    average = jnp.mean(projected, axis=-1, keepdims=True)
    centered = projected - average
    spread = jnp.mean(centered * centered, axis=-1, keepdims=True)
    normed = centered * lax.rsqrt(spread + norm_epsilon) * gain_ref[...] + shift_ref[...]
    for w in range(windows):
        for half, out_ref in ((0, out_own_ref), (1, out_halo_ref)):
            start = w * WIN_TOK + half * HALF_TOK
            size = HALF_TOK if w < windows - 1 else BLOCK
            out_ref[w * HALF_TOK:w * HALF_TOK + size] = normed[start:start + size].astype(jnp.bfloat16)
            if w == windows - 1:
                out_last_ref[half] = normed[start + BLOCK:start + HALF_TOK].astype(jnp.bfloat16)


def whole(a):
    return pl.BlockSpec(a.shape, lambda i: (0,) * a.ndim)


def attend(own, own_last, halo, halo_last, z, w_qkv, bias, codes, w_proj, proj_bias, norm_gain, norm_shift):
    features = own.shape[-1]
    main_bias, rest_bias = bias
    windows = main_bias.shape[0]
    bias_spec = pl.BlockSpec((windows, None, HEADS, WIN_TOK, LANES), lambda i: (0, z, 0, 0, 0))
    part_spec = pl.BlockSpec((None,) + own.shape[1:], lambda i: (z, 0, 0))
    halo_spec = pl.BlockSpec((None,) + halo.shape[1:], lambda i: (z, 0, 0))
    own_last_spec = pl.BlockSpec((None, None) + own_last.shape[2:], lambda i: (z, 1, 0, 0))
    halo_last_spec = pl.BlockSpec((None,) + halo_last.shape[1:], lambda i: (z, 0, 0))
    rows = [v.reshape(1, features) for v in (proj_bias, norm_gain, norm_shift)]
    args = (own, own_last, halo, halo_last, w_qkv, main_bias, rest_bias, codes[0][z], codes[1][z], w_proj, *rows)
    specs = [part_spec, own_last_spec, halo_spec, halo_last_spec, whole(w_qkv), bias_spec, bias_spec]
    specs += [whole(a) for a in args[len(specs):]]
    out = jax.ShapeDtypeStruct(own.shape[1:], jnp.bfloat16)
    out_last = jax.ShapeDtypeStruct((2, BLOCK, features), jnp.bfloat16)
    width = HEADS * HEAD_DIM
    return pl.pallas_call(
        attend_kernel,
        out_shape=(out, out, out_last),
        grid=(1,),
        in_specs=specs,
        out_specs=[whole(out), whole(out), whole(out_last)],
        scratch_shapes=[
            pltpu.VMEM((windows * WIN_TOK, 3 * width), jnp.float32),
            pltpu.VMEM((windows * WIN_TOK, width), jnp.bfloat16),
        ],
        compiler_params=pltpu.CompilerParams(vmem_limit_bytes=48 << 20),
        cost_estimate=pl.CostEstimate(
            flops=6 * 10 ** 9, transcendentals=10 ** 6, bytes_accessed=8 << 20
        ),
        name="window_attention",
    )(*args)


def shifted_levels(z, levels):
    return [(WIN_Z * z + d + WIN_Z // 2) % levels for d in range(WIN_Z)]


def pack_kernel(state_ref, mask_ref, embed_ref, chosen_ref, first_ref, own_ref, last_ref, hidden_ref):
    levels, lat_rows, columns, features = state_ref.shape
    groups = lat_rows // (WIN_LAT // 2)
    starts, _ = offsets(groups)
    kept = first_ref.shape[1]
    hidden_ref[...] = jnp.zeros_like(hidden_ref)
    for i in range(lat_rows):
        embedded = jnp.where(mask_ref[:, i:i + 1] == 1, embed_ref[1:2], embed_ref[0:1])
        for z in range(levels):
            hidden = (state_ref[z, i].astype(jnp.float32) + embedded).astype(jnp.bfloat16)
            hidden_ref[z, i, :columns] = hidden
    for z in range(levels // WIN_Z):
        slabs = [
            hidden_ref[l].reshape(lat_rows * SLAB, features) for l in shifted_levels(z, levels)
        ]
        packed = jnp.dot(
            chosen_ref[...], jnp.concatenate(slabs, axis=0), preferred_element_type=jnp.float32
        ).astype(jnp.bfloat16)
        first_ref[z] = packed[:kept]
        last_ref[z, 0] = packed[starts[1]:starts[1] + BLOCK]
        own_ref[z] = packed[starts[2]:starts[2] + kept]
        last_ref[z, 1] = packed[starts[3]:starts[3] + BLOCK]


def pack(state_tokens, land_mask, land_embed):
    levels, lat_rows, _, features = state_tokens.shape
    z_windows = levels // WIN_Z
    kept = (lat_rows // (WIN_LAT // 2) - 1) * BLOCK
    part = jax.ShapeDtypeStruct((z_windows, kept, features), jnp.bfloat16)
    return pl.pallas_call(
        pack_kernel,
        out_shape=(
            part, part,
            jax.ShapeDtypeStruct((z_windows, 2, BLOCK, features), jnp.bfloat16),
            jax.ShapeDtypeStruct((levels, lat_rows, SLAB, features), jnp.bfloat16),
        ),
        compiler_params=pltpu.CompilerParams(vmem_limit_bytes=32 << 20),
        name="embed_and_pack",
    )(state_tokens, land_mask.T, land_embed, jnp.asarray(packing(lat_rows), jnp.bfloat16))


def unpack_kernel(hidden_ref, chosen_ref, *refs):
    result_ref, packed_ref = refs[-2:]
    levels, lat_rows, columns, features = result_ref.shape
    starts, _ = offsets(lat_rows // (WIN_LAT // 2))
    packed_ref[...] = jnp.zeros_like(packed_ref)
    for z in range(levels // WIN_Z):
        for start, ref in zip(starts, refs[4 * z:4 * z + 4]):
            packed_ref[z, start:start + ref.shape[0]] = ref[...]
        placed = jnp.dot(chosen_ref[...], packed_ref[z], preferred_element_type=jnp.float32)
        for d, l in enumerate(shifted_levels(z, levels)):
            rows = lat_rows * SLAB
            hidden = hidden_ref[l].reshape(rows, features).astype(jnp.float32)
            total_rows = (hidden + placed[d * rows:(d + 1) * rows]).astype(jnp.bfloat16)
            result_ref[l] = total_rows.reshape(lat_rows, SLAB, features)[:, :columns]


def unpack(hidden, parts, shape):
    levels, lat_rows, _, features = shape
    _, total = offsets(lat_rows // (WIN_LAT // 2))
    return pl.pallas_call(
        unpack_kernel,
        out_shape=jax.ShapeDtypeStruct(shape, jnp.bfloat16),
        scratch_shapes=[pltpu.VMEM((levels // WIN_Z, total, features), jnp.bfloat16)],
        compiler_params=pltpu.CompilerParams(vmem_limit_bytes=32 << 20),
        name="unpack_and_add",
    )(hidden, jnp.asarray(packing(lat_rows).T, jnp.bfloat16), *parts)


def on_device(
    state_tokens,
    land_mask,
    pad_mask,
    land_embed,
    w_qkv,
    w_proj,
    proj_bias,
    norm_gain,
    norm_shift,
    bias_table,
    index_table,
):
    levels, lat_rows, _, _ = state_tokens.shape
    lat_total = lat_rows * lax.axis_size("lat")
    lat_start = lax.axis_index("lat") * lat_rows
    z_windows = levels // WIN_Z
    first, own, last, hidden = pack(state_tokens, land_mask, land_embed)
    halo = from_behind(first, "lon", -1)
    last = from_behind(last, "lat", -1)
    halo_last = from_behind(last[:, 0], "lon", -1)
    bias = earth_bias(bias_table, index_table)
    codes = window_rules(levels, lat_start, lat_rows, lat_total, pad_mask)
    kept, returned, lasts = [], [], []
    for z in range(z_windows):
        own_out, halo_out, last_out = attend(
            own, last, halo, halo_last, z, w_qkv, bias, codes,
            w_proj, proj_bias, norm_gain, norm_shift,
        )
        kept.append(own_out)
        returned.append(from_behind(halo_out, "lon", 1))
        lasts.append(last_out)
    turned = from_behind(jnp.stack(lasts), "lat", 1)
    corner = from_behind(turned[:, 1], "lon", 1)
    parts = []
    for z in range(z_windows):
        parts += [returned[z], corner[z], kept[z], turned[z, 0]]
    return unpack(hidden, parts, state_tokens.shape)


def solution(mesh):
    in_specs = (
        P("member", "lat", "lon", None),
        P("lat", "lon"),
        P(),
        P(),
        P(),
        P(),
        P(),
        P(),
        P(),
        P("lat", None, None, None),
        P(),
    )
    out_specs = P("member", "lat", "lon", None)
    return jax.shard_map(
        on_device, mesh=mesh, in_specs=in_specs, out_specs=out_specs, check_vma=False
    )
```
